256 devices in a mesh: outer: 4 (over y), dev: 64 (over x, z, core).
Axes of the slice: x: 4, y: 4, z: 8, core: 2. Of those that a mesh axis runs over, the one named last changes fastest.
Arguments:
- documents: bfloat16 [49152, 4096], P(('outer', 'dev')), may hold values from -8 to 8
- cluster_of: int32 [49152], replicated, may hold values from 0 to 255, as said below
- neighbours: int32 [256, 4], replicated, may hold values from 0 to 255, as said below
- sharpness: float32 [256], replicated, may hold values from 32 to 64
Outputs:
- density: float32 [49152], P(('outer', 'dev'))
The draws below stay inside these ranges and needn't reach their ends.
Inputs may be any that keep to these rules, and one draw needn't show every extreme that they name: `cluster_of`: rows b * 192 to (b + 1) * 192 - 1 form block b. Block b names only clusters g * 64 to (g + 1) * 64 - 1, with g = b // 64, and names no cluster more than 6 times; in each group g some cluster is named exactly 6 times by every block of that group; every cluster is named by some row. `neighbours`: row c, with c = g * 64 + h, lists in order the clusters g * 64 + ((h - 1) mod 64), g * 64 + ((h + 1) mod 64), ((g - 1) mod 4) * 64 + ((h + b) mod 64) and ((g + 1) mod 4) * 64 + ((h + d) mod 64), with b and d each in -1, 0, 1.
All inputs are finite; a program needn't handle non-finite values.
Results may differ from the reference program's by a relative error of at most 0.00047.
Values may be sent and summed in bfloat16 or wider, within the bound.
No kernel may reach another device: no remote copies, remote signals or barrier semaphores. Data moves between devices by JAX's collectives and lax.ppermute only.
A program may use at most 128 MiB of HBM per device.

```python
import math
import jax
import jax.numpy as jnp
from jax import lax

E = 4096
NEIGHBOURS = 4
TOK_DEV = 192
CLUSTER_GROUPS = 4
CLUSTERS_IN_GROUP = 64
CLUSTERS = 256
CAP = 6
SLOTS = 384
DOCS = 49152


theme_count = 32


def cluster_draw(key):
    blocks_total = CLUSTER_GROUPS * CLUSTERS_IN_GROUP
    tickets = CLUSTERS_IN_GROUP * CAP
    base_key = jax.random.fold_in(key, 7)
    split_points = jax.random.split(base_key, 4)
    extra_reward = jax.random.randint(split_points[0], (CLUSTER_GROUPS, CLUSTERS_IN_GROUP), 0, 4096)
    weighty_blocks = jax.random.randint(split_points[1], (CLUSTER_GROUPS,), 0, CLUSTERS_IN_GROUP)
    extra_reward = jnp.where(jnp.arange(CLUSTERS_IN_GROUP, dtype=jnp.int32)[None, :] == weighty_blocks[:, None], 32768, extra_reward)
    owner_of_ticket = jnp.arange(tickets, dtype=jnp.int32) // CAP
    ticket_copy = jnp.arange(tickets, dtype=jnp.int32) % CAP
    random_perturb = jax.random.randint(split_points[2], (blocks_total, tickets), 0, 4096)
    group_of_block = jnp.arange(blocks_total, dtype=jnp.int32) // CLUSTERS_IN_GROUP
    block_owner = jnp.arange(blocks_total, dtype=jnp.int32) % CLUSTERS_IN_GROUP
    compelled_choice = (owner_of_ticket[None, :] == block_owner[:, None]) & (ticket_copy[None, :] == 0)
    density_scores = random_perturb + extra_reward[group_of_block][:, owner_of_ticket] + jnp.where(compelled_choice, 65536, 0)
    density_scores = density_scores * tickets + jnp.arange(tickets, dtype=jnp.int32)[None, :]
    ranked, chosen = lax.top_k(density_scores, TOK_DEV)
    local_labels = owner_of_ticket[chosen]
    shuffled = jax.random.permutation(split_points[3], local_labels, axis=1, independent=True)
    labels_all = shuffled + group_of_block[:, None] * CLUSTERS_IN_GROUP
    return labels_all.reshape(-1).astype(jnp.int32)


def draw_cluster_of(key, part):
    return cluster_draw(key)


def draw_documents(key, part):
    labels_all = cluster_draw(key)
    base_key = jax.random.fold_in(key, 13)
    split_points = jax.random.split(base_key, 4)
    centres = jax.random.normal(split_points[0], (CLUSTERS, E), jnp.float32)
    themes = jax.random.normal(split_points[1], (theme_count, E), jnp.float32)
    picked = jax.random.randint(split_points[2], (DOCS,), 0, theme_count)
    noise = jax.random.normal(split_points[3], (DOCS, E), jnp.float32)
    theme_weight = 0.35
    values = centres[labels_all] + theme_weight * themes[picked] + noise
    return jnp.clip(values, -8.0, 8.0).astype(jnp.bfloat16)


def draw_neighbours(key, part):
    base_key = jax.random.fold_in(key, 17)
    offsets = jax.random.randint(base_key, (CLUSTERS, 2), -1, 2).astype(jnp.int32)
    cluster_range = jnp.arange(CLUSTERS, dtype=jnp.int32)
    group_of = cluster_range // CLUSTERS_IN_GROUP
    owner_of = cluster_range % CLUSTERS_IN_GROUP
    group_moves = jnp.stack([jnp.zeros_like(group_of), jnp.zeros_like(group_of), jnp.full_like(group_of, -1), jnp.ones_like(group_of)], axis=1)
    owner_moves = jnp.stack([jnp.full_like(owner_of, -1), jnp.ones_like(owner_of), offsets[:, 0], offsets[:, 1]], axis=1)
    group_next = (group_of[:, None] + group_moves + CLUSTER_GROUPS) % CLUSTER_GROUPS
    owner_next = (owner_of[:, None] + owner_moves + CLUSTERS_IN_GROUP) % CLUSTERS_IN_GROUP
    return (group_next * CLUSTERS_IN_GROUP + owner_next).astype(jnp.int32)


def setup_inputs(seed: int = 0) -> dict:
    key_of = jax.random.split(jax.random.key(seed), 5)
    return {
        "documents": draw_documents(jax.random.fold_in(key_of[4], 71), 0),
        "cluster_of": draw_cluster_of(jax.random.fold_in(key_of[4], 71), 0),
        "neighbours": draw_neighbours(jax.random.fold_in(key_of[4], 71), 0),
        "sharpness": jnp.clip(jnp.exp(jax.random.uniform(key_of[3], (CLUSTERS,), jnp.float32, math.log(32.0), math.log(64.0))), 32.0, 64.0),
    }


def reference(documents, cluster_of, neighbours, sharpness):
    count_blocks = DOCS // TOK_DEV
    cluster_sizes = jnp.zeros((CLUSTERS,), jnp.int32).at[cluster_of].add(1)
    cluster_sums = jax.ops.segment_sum(documents.astype(jnp.float32), cluster_of, num_segments=CLUSTERS)
    cluster_means = cluster_sums / cluster_sizes.astype(jnp.float32)[:, None]
    centred = documents.astype(jnp.float32) - cluster_means[cluster_of]
    scaling = lax.rsqrt(lax.optimization_barrier(jnp.mean(centred * centred, axis=1)) + 1e-06) / math.sqrt(E)
    unit_rows = (centred * scaling[:, None]).astype(jnp.bfloat16)
    block_labels = cluster_of.reshape(count_blocks, TOK_DEV)
    ordinal = jnp.arange(TOK_DEV, dtype=jnp.int32)
    earlier = ordinal[None, :] < ordinal[:, None]
    repeats = lax.optimization_barrier(jnp.sum(((block_labels[:, :, None] == block_labels[:, None, :]) & earlier[None]).astype(jnp.int32), axis=2))
    source_slot = (jnp.arange(count_blocks, dtype=jnp.int32) % CLUSTERS_IN_GROUP)[:, None]
    slot_of = (source_slot * CAP + repeats).reshape(-1).astype(jnp.int32)
    rows_index = jnp.arange(DOCS, dtype=jnp.int32)
    slot_table = jnp.zeros((CLUSTERS, SLOTS), jnp.int32).at[cluster_of, slot_of].set(rows_index)
    filled = jnp.zeros((CLUSTERS, SLOTS), jnp.float32).at[cluster_of, slot_of].set(1.0)
    off_diagonal = 1.0 - jnp.eye(SLOTS, dtype=jnp.float32)

    def per_cluster(cluster_index):
        queries = unit_rows[slot_table[cluster_index]]
        own_gain = sharpness[cluster_index]
        own_terms = jnp.exp(own_gain * jnp.dot(queries, queries.T, preferred_element_type=jnp.float32))
        running = lax.optimization_barrier(jnp.sum(own_terms * filled[cluster_index][None, :] * off_diagonal, axis=1))
        for position in range(NEIGHBOURS):
            partner = neighbours[cluster_index, position]
            key_rows = unit_rows[slot_table[partner]]
            pair_gain = 0.5 * (own_gain + sharpness[partner])
            kernel_terms = jnp.exp(pair_gain * jnp.dot(queries, key_rows.T, preferred_element_type=jnp.float32))
            running = running + lax.optimization_barrier(jnp.sum(kernel_terms * filled[partner][None, :], axis=1))
        partner_count = cluster_sizes[cluster_index] - 1 + jnp.sum(cluster_sizes[neighbours[cluster_index]])
        return jnp.log(running / partner_count.astype(jnp.float32))
    slot_density = lax.map(per_cluster, jnp.arange(CLUSTERS, dtype=jnp.int32))
    return slot_density[cluster_of, slot_of]
```

```python
import functools

import numpy as np
import jax
import jax.numpy as jnp
from jax import lax
from jax.experimental import pallas as pl
from jax.experimental.pallas import tpu as pltpu
from jax.sharding import PartitionSpec as P

GROUPS, OWNERS, CAP, WIDTH, TOK = 4, 64, 6, 4096, 192
SLOTS = OWNERS * CAP
SPLIT = 4
CHUNKS = (1024, 1024, 1024, 1024)
BATCH = 4
PART = SLOTS // BATCH


_d = np.arange(OWNERS)
_x, _z, _c = _d // 16, (_d // 2) % 8, _d % 2
LABEL = 2 * (4 * _z + np.where(_z % 2 == 0, _x, 3 - _x)) + _c
PLACE = np.argsort(LABEL)


def label_of(device):
    x, z, core = device // 16, (device // 2) % 8, device % 2
    return 2 * (4 * z + jnp.where(z % 2 == 0, x, 3 - x)) + core


def place_of(label):
    chip, core = label // 2, label % 2
    z, along = chip // 4, chip % 4
    return (jnp.where(z % 2 == 0, along, 3 - along) * 8 + z) * 2 + core


def along_ring(block, step):
    route = [(int(PLACE[(h - step) % OWNERS]), int(PLACE[h])) for h in range(OWNERS)]
    return lax.ppermute(block, "dev", route)


def along_outer(block, step):
    return lax.ppermute(block, "outer", [((i - step) % GROUPS, i) for i in range(GROUPS)])


def unpack_kernel(arrived, raw):
    rows = SPLIT * PART
    for q in range(SPLIT):
        slot = lax.broadcasted_iota(jnp.int32, (PART, rows), 0)
        line = lax.broadcasted_iota(jnp.int32, (PART, rows), 1)
        choose = jnp.where(line == slot * SPLIT + q, 1.0, 0.0).astype(jnp.bfloat16)
        for b in range(BATCH):
            raw[q, b * PART : (b + 1) * PART, :] = jnp.dot(
                choose, arrived[b * rows : (b + 1) * rows, :], preferred_element_type=jnp.float32
            ).astype(jnp.bfloat16)


def unpacked(arrived):
    width = arrived.shape[1]
    return pl.pallas_call(
        unpack_kernel,
        out_shape=jax.ShapeDtypeStruct((SPLIT, SLOTS, width), jnp.bfloat16),
        cost_estimate=pl.CostEstimate(
            flops=2 * SLOTS * SPLIT * SLOTS * width, bytes_accessed=4 * SLOTS * SPLIT * width, transcendentals=0
        ),
        name="unpack",
    )(arrived)


def unit_rows(raws, unit, size):
    squares = jnp.zeros((SLOTS, 1), jnp.float32)
    means = []
    for raw in raws:
        for q in range(SPLIT):
            rows = raw[q].astype(jnp.float32)
            mean = jnp.sum(rows, axis=0, keepdims=True) / size
            means.append(mean)
            centred = rows - mean
            squares = squares + jnp.sum(centred * centred, axis=1, keepdims=True)
    scaling = lax.rsqrt(squares / WIDTH + 1e-06) / (WIDTH**0.5)
    at, block = 0, 0
    for raw in raws:
        width = raw.shape[2]
        for q in range(SPLIT):
            centred = raw[q].astype(jnp.float32) - means[block]
            unit[:, at : at + width] = (centred * scaling).astype(jnp.bfloat16)
            at, block = at + width, block + 1


def products(queries, keys):
    return lax.dot_general(
        queries[...], keys[...], (((1,), (1,)), ((), ())), preferred_element_type=jnp.float32
    )


def own_kernel(scalars, mask, *refs):
    raws, (unit, total) = refs[: len(CHUNKS)], refs[len(CHUNKS) :]
    unit_rows(raws, unit, scalars[0])
    terms = jnp.exp(scalars[1] * products(unit, unit))
    row = lax.broadcasted_iota(jnp.int32, (SLOTS, SLOTS), 0)
    column = lax.broadcasted_iota(jnp.int32, (SLOTS, SLOTS), 1)
    kept = (mask[...] > 0.0) & (row != column)
    total[...] = jnp.sum(jnp.where(kept, terms, 0.0), axis=1, keepdims=True)


def cross_kernel(scalars, mask, queries, *refs):
    raws, (total, unit) = refs[: len(CHUNKS)], refs[len(CHUNKS) :]
    unit_rows(raws, unit, scalars[0])
    terms = jnp.exp(scalars[1] * products(queries, unit))
    total[...] = jnp.sum(jnp.where(mask[...] > 0.0, terms, 0.0), axis=1, keepdims=True)


COST = pl.CostEstimate(
    flops=2 * SLOTS * SLOTS * WIDTH, bytes_accessed=6 * SLOTS * WIDTH, transcendentals=SLOTS * SLOTS
)
SMEM = pl.BlockSpec(memory_space=pltpu.SMEM)
VMEM = pl.BlockSpec(memory_space=pltpu.VMEM)


def own_block(scalars, mask, raws):
    return pl.pallas_call(
        own_kernel,
        in_specs=[SMEM] + [VMEM] * (1 + len(raws)),
        out_shape=(
            jax.ShapeDtypeStruct((SLOTS, WIDTH), jnp.bfloat16),
            jax.ShapeDtypeStruct((SLOTS, 1), jnp.float32),
        ),
        cost_estimate=COST,
        name="own",
    )(scalars, mask, *raws)


def cross_block(scalars, mask, queries, raws):
    return pl.pallas_call(
        cross_kernel,
        in_specs=[SMEM] + [VMEM] * (2 + len(raws)),
        out_shape=jax.ShapeDtypeStruct((SLOTS, 1), jnp.float32),
        scratch_shapes=[pltpu.VMEM((SLOTS, WIDTH), jnp.bfloat16)],
        cost_estimate=COST,
        name="cross",
    )(scalars, mask, queries, *raws)


def shards(documents, cluster_of, neighbours, sharpness):
    group = lax.axis_index("outer")
    device = lax.axis_index("dev")
    label = label_of(device)
    own = group * OWNERS + label

    labels_here = lax.dynamic_slice(cluster_of, ((group * OWNERS + device) * TOK,), (TOK,)) - group * OWNERS
    ordinal = jnp.arange(TOK, dtype=jnp.int32)
    earlier = ordinal[None, :] < ordinal[:, None]
    repeats = jnp.sum(((labels_here[:, None] == labels_here[None, :]) & earlier).astype(jnp.int32), axis=1)
    target = place_of(labels_here) * CAP + repeats

    line = jnp.arange(SLOTS * SPLIT, dtype=jnp.int32)[:, None]
    column_target = jnp.concatenate([target * SPLIT + q for q in range(SPLIT)])
    placing = (line == column_target[None, :]).astype(jnp.bfloat16)

    starts = [sum(CHUNKS[:i]) for i in range(len(CHUNKS))]
    own_raw, left_raw, right_raw, below_raw, above_raw = [], [], [], [], []
    moves = []
    for direction, position in ((1, 2), (-1, 3)):
        receiver = (group + direction) % GROUPS
        wanted = neighbours[receiver * OWNERS + label, position]
        moves.append((wanted % OWNERS - label + OWNERS) % OWNERS)
    for start, width in zip(starts, CHUNKS):
        part = width // SPLIT
        stacked = jnp.concatenate(
            [documents[:, start + q * part : start + (q + 1) * part] for q in range(SPLIT)], axis=0
        )
        outgoing = jnp.dot(placing, stacked, preferred_element_type=jnp.float32).astype(jnp.bfloat16)
        arrived = lax.all_to_all(
            outgoing.reshape(OWNERS, CAP * SPLIT, part), "dev", split_axis=0, concat_axis=0, tiled=True
        ).reshape(SLOTS * SPLIT, part)
        raw = unpacked(arrived)
        left, right = along_ring(raw, 1), along_ring(raw, -1)
        own_raw.append(raw)
        left_raw.append(left)
        right_raw.append(right)
        for moved, direction, kept in ((moves[0], 1, below_raw), (moves[1], -1, above_raw)):
            picked = jnp.where(moved == 1, right, jnp.where(moved == OWNERS - 1, left, raw))
            kept.append(along_outer(picked, direction))

    block_labels = cluster_of.reshape(GROUPS, OWNERS, TOK) - (
        jnp.arange(GROUPS, dtype=jnp.int32) * OWNERS
    )[:, None, None]
    per_block = jnp.sum(
        (block_labels[..., None] == jnp.arange(OWNERS, dtype=jnp.int32)).astype(jnp.int32), axis=2
    )
    sizes = jnp.sum(per_block, axis=1).reshape(-1)
    listed = neighbours[own]
    gain = sharpness[own]
    slot = jnp.arange(CAP, dtype=jnp.int32)

    def mask_of(cluster):
        senders = per_block[cluster // OWNERS, :, cluster % OWNERS]
        return (slot[None, :] < senders[:, None]).astype(jnp.float32).reshape(1, SLOTS)

    def scalars_of(cluster):
        return jnp.stack([sizes[cluster].astype(jnp.float32), 0.5 * (gain + sharpness[cluster])])

    unit, running = own_block(scalars_of(own), mask_of(own), own_raw)
    for position, raws in enumerate((left_raw, right_raw, below_raw, above_raw)):
        partner = listed[position]
        running = running + cross_block(scalars_of(partner), mask_of(partner), unit, raws)
    partner_count = sizes[own] - 1 + jnp.sum(sizes[listed])
    slot_density = jnp.log(running[:, 0] / partner_count.astype(jnp.float32))
    answered = lax.all_to_all(
        slot_density.reshape(OWNERS, CAP), "dev", split_axis=0, concat_axis=0, tiled=True
    ).reshape(-1)
    return answered[target]


def solution(mesh):
    in_specs = (P(("outer", "dev"), None), P(), P(), P())
    out_specs = P(("outer", "dev"))
    return jax.shard_map(shards, mesh=mesh, in_specs=in_specs, out_specs=out_specs, check_vma=False)
```
